32 devices in a mesh: blk: 32 (over z, y, x, core).
Axes of the slice: x: 2, y: 2, z: 4, core: 2. Of those that a mesh axis runs over, the one named last changes fastest.
Arguments:
- frames: float32 [128, 128, 1280], P('blk'), may hold values from -6 to 6
- widths: float32 [128], replicated, may hold values from 2 to 12
- kernel: float32 [3, 3], replicated, may hold values from -3 to 3
Outputs:
- filtered: float32 [128, 128, 1280], P(None, 'blk')
The draws below stay inside these ranges and needn't reach their ends.
All inputs are finite; a program needn't handle non-finite values.
Results may differ from the reference program's by a relative error of at most 0.00007.
Values sent between devices are 32-bit elements; how exact they have to be, the bound alone decides.
A program may use at most 64 MiB of HBM per device.

```python
import math
import jax
import jax.numpy as jnp
from jax import lax

FRAMES = 128
BAND = 24
W = 1280
H = 128


def block_scale(key, shape, pieces, least, top_value):
    factor_of, own = 1.0, jax.random.fold_in(key, 6)
    for axis_at, shards_of in pieces:
        heights = jnp.exp(jax.random.uniform(jax.random.fold_in(own, axis_at), (shards_of,), jnp.float32, least / len(pieces), top_value / len(pieces)))
        factor_of = factor_of * jnp.repeat(heights, shape[axis_at] // shards_of).reshape([-1 if axis == axis_at else 1 for axis in range(len(shape))])
    return factor_of


def normal_values(key, extent, scale, most, cuts=(), kind=jnp.bfloat16):
    values = scale * jax.random.normal(key, extent, jnp.float32)
    if cuts:
        values = values * block_scale(key, extent, cuts, -0.22, 0.18)
    return jnp.clip(values, -most, most).astype(kind)


def setup_inputs(seed: int = 0) -> dict:
    key_of = jax.random.split(jax.random.key(seed), 4)
    frames = normal_values(key_of[0], (FRAMES, H, W), 1.0, 6.0, ((0, 32),), jnp.float32)
    widths = jnp.clip(jnp.exp(jax.random.uniform(key_of[1], (FRAMES,), jnp.float32, math.log(2.0), math.log(12.0))), 2.0, 12.0)
    kernel = normal_values(key_of[2], (3, 3), 0.5, 3.0, (), jnp.float32)
    return dict(frames=frames, widths=widths, kernel=kernel)


def temporal_matrix(widths, length):
    steps = jnp.arange(length, dtype=jnp.int32)
    offset = (steps[:, None] - steps[None, :]).astype(jnp.float32)
    inside = jnp.abs(offset) <= BAND
    spread = widths.astype(jnp.float32)[:, None]
    weights = jnp.where(inside, jnp.exp(-offset * offset / (2.0 * spread * spread)), 0.0)
    return weights / jnp.sum(weights, axis=1, keepdims=True)


def stencil(padded, kernel):
    rows_out = padded.shape[1] - 2
    columns = padded.shape[2]
    widened = jnp.pad(padded, ((0, 0), (0, 0), (1, 1)))
    summed = jnp.zeros((padded.shape[0], rows_out, columns), jnp.float32)
    for row_off in range(3):
        for col_off in range(3):
            summed = summed + kernel[row_off, col_off] * widened[:, row_off:row_off + rows_out, col_off:col_off + columns]
    return summed


def reference(frames, widths, kernel):
    weights = temporal_matrix(widths, frames.shape[0])
    smoothed = jnp.einsum("ts,srw->trw", weights, frames, precision=lax.Precision.HIGHEST)
    padded = jnp.pad(smoothed, ((0, 0), (1, 1), (0, 0)))
    return stencil(padded, kernel)
```

```python
import functools

import jax
import jax.numpy as jnp
from jax import lax
from jax.experimental import pallas as pl
from jax.experimental.pallas import tpu as pltpu
from jax.sharding import PartitionSpec as P

BAND = 24
MESH = pl.DeviceIdType.MESH


def exchange_kernel(
    n,
    frames_ref,
    widths_hbm,
    kernel_hbm,
    out_ref,
    held,
    window,
    outgoing,
    incoming,
    mixing,
    widths_ref,
    kernel_ref,
    in_sem,
    send_sem,
    recv_sem,
    relay_sem,
):
    per_device, height, columns = frames_ref.shape
    chunks, _, rows_block, chunk = outgoing.shape
    rows = rows_block // per_device
    group = 8 // rows
    groups = n // group
    length = widths_ref.shape[1]
    me = lax.axis_index("blk")
    quarter = n // 4
    mine = me // quarter
    place = me - mine * quarter
    mirror = 3 - mine
    beside = mine + 1 - 2 * lax.rem(mine, 2)
    across = mirror + 1 - 2 * lax.rem(mirror, 2)
    partner = beside * quarter + place
    opposite = mirror * quarter + place

    strip = height // 4
    first = mirror * strip
    above = jnp.where(mirror == 0, 0, first - 8)
    below = jnp.where(mirror == 3, height - 8, first + strip)

    def load(source, rows_in, target, at, semaphore):
        return pltpu.make_async_copy(
            frames_ref.at[:, pl.ds(pl.multiple_of(source, 8), rows_in), :],
            target.at[:, pl.ds(at, rows_in), :],
            semaphore,
        )

    early = [
        pltpu.make_async_copy(kernel_hbm, kernel_ref, in_sem.at[1]),
        load(first, strip, window, 8, in_sem.at[3]),
        load(above, 8, window, 0, in_sem.at[4]),
        load(below, 8, window, strip + 8, in_sem.at[5]),
    ]
    late = [
        load(0, height, held, 8, in_sem.at[0]),
        pltpu.make_async_copy(widths_hbm, widths_ref, in_sem.at[2]),
    ]
    for copy in early:
        copy.start()

    def signal(semaphore, target):
        pl.semaphore_signal(
            semaphore, inc=1, device_id=(target,), device_id_type=MESH
        )

    barrier = pltpu.get_barrier_semaphore()

    @pl.loop(0, quarter)
    def _(step):
        signal(barrier, mirror * quarter + lax.rem(place + step, quarter))

    signal(barrier, partner)

    edge = jnp.zeros((per_device, 8, columns), jnp.float32)
    held[:, pl.ds(0, 8), :] = edge
    held[:, pl.ds(height + 8, 8), :] = edge
    for copy in early:
        copy.wait()
    for copy in late:
        copy.start()

    @pl.when(mirror == 0)
    def _():
        window[:, pl.ds(0, 8), :] = edge

    @pl.when(mirror == 3)
    def _():
        window[:, pl.ds(strip + 8, 8), :] = edge

    part = quarter // group
    own = me // group
    seat = place // group

    def group_at(which, step):
        return which * part + lax.rem(seat + step, part)

    column = lax.broadcasted_iota(jnp.int32, (8, columns), 1)

    def filter_group(at, source, base):
        for frame in range(per_device):
            tall = source[frame, pl.ds(pl.multiple_of((at - base) * 8, 8), 24), :]
            taps = [tall[7:15], tall[8:16], tall[9:17]]
            mixed = [
                kernel_ref[0, col] * taps[0]
                + kernel_ref[1, col] * taps[1]
                + kernel_ref[2, col] * taps[2]
                for col in range(3)
            ]
            left = jnp.where(column == 0, 0.0, pltpu.roll(mixed[0], 1, 1))
            right = jnp.where(
                column == columns - 1, 0.0, pltpu.roll(mixed[2], columns - 1, 1)
            )
            value = left + mixed[1] + right
            for member in range(group):
                for k in range(chunks):
                    outgoing[
                        k, at * group + member, pl.ds(frame * rows, rows), :
                    ] = value[
                        member * rows : (member + 1) * rows,
                        k * chunk : (k + 1) * chunk,
                    ]

    def send(k, target):
        pltpu.make_async_remote_copy(
            src_ref=outgoing.at[k, target],
            dst_ref=incoming.at[k, me],
            send_sem=send_sem.at[k],
            recv_sem=recv_sem.at[k],
            device_id=(target,),
            device_id_type=MESH,
        ).start()

    def send_own_group(k):
        for other in range(1, group):
            send(k, own * group + lax.rem(me + other, group))
        pltpu.make_async_copy(
            outgoing.at[k, me], incoming.at[k, me], recv_sem.at[k]
        ).start()

    def filter_quarter(which):
        @pl.loop(0, part)
        def _(step):
            filter_group(group_at(which, step), held, 0)

    def send_quarter(which, k):
        @pl.loop(0, part)
        def _(step):
            at = group_at(which, step)
            for member in range(group):
                send(k, at * group + member)

    def send_near(k):
        @pl.loop(1, part)
        def _(step):
            at = group_at(mine, step)
            for member in range(group):
                send(k, at * group + member)

        send_own_group(k)

    def filter_early(step):
        filter_group(group_at(mirror, step), window, mirror * part)

    def send_early(step):
        at = group_at(mirror, step)

        @pl.loop(0, opening)
        def _(k):
            for member in range(group):
                send(k, at * group + member)

    opening = min(2, chunks)
    inner = (mine == 1) | (mine == 2)
    filter_early(0)
    pl.semaphore_wait(barrier, quarter + 1)
    signal(relay_sem.at[0], partner)

    @pl.loop(0, part - 1)
    def _(step):
        send_early(step)
        filter_early(step + 1)

    send_early(part - 1)
    for copy in late:
        copy.wait()
    filter_quarter(across)
    pl.semaphore_wait(relay_sem.at[0], 1)
    signal(relay_sem.at[1], opposite)

    def send_mirror():
        @pl.loop(opening, chunks)
        def _(k):
            send_quarter(mirror, k)

    def send_across():
        @pl.loop(0, chunks)
        def _(k):
            send_quarter(across, k)

    pl.when(inner)(send_across)
    pl.when(jnp.logical_not(inner))(send_mirror)
    filter_quarter(beside)
    filter_quarter(mine)
    pl.semaphore_wait(relay_sem.at[1], 1)

    @pl.loop(0, chunks)
    def _(k):
        send_quarter(beside, k)
        send_near(k)

    pl.when(inner)(send_mirror)
    pl.when(jnp.logical_not(inner))(send_across)

    total = length * rows
    target_at = lax.broadcasted_iota(jnp.int32, (total, length), 0) // rows
    lane = lax.broadcasted_iota(jnp.int32, (total, length), 1)
    spread = jnp.sum(
        jnp.where(target_at == lane, widths_ref[...], 0.0), axis=1, keepdims=True
    )
    row_at = lax.broadcasted_iota(jnp.int32, (total, total), 0)
    col_at = lax.broadcasted_iota(jnp.int32, (total, total), 1)
    apart = row_at // rows - col_at // rows
    inside = (jnp.abs(apart) <= BAND) & (row_at % rows == col_at % rows)
    offset = apart.astype(jnp.float32)
    weights = jnp.where(
        inside, jnp.exp(-offset * offset / (2.0 * spread * spread)), 0.0
    )
    mixing[...] = weights / jnp.sum(weights, axis=1, keepdims=True)

    @pl.loop(0, chunks)
    def _(k):
        pltpu.make_async_copy(incoming.at[k], incoming.at[k], recv_sem.at[k]).wait()
        if rows_block % 8 == 0:
            block = incoming[k].reshape(total, chunk)
        else:
            block = jnp.concatenate([incoming[k, s] for s in range(n)], axis=0)
        mixed = jnp.dot(
            mixing[...],
            block,
            precision=lax.Precision.HIGHEST,
            preferred_element_type=jnp.float32,
        )
        out_ref[:, :, pl.ds(pl.multiple_of(k * chunk, 128), chunk)] = mixed.reshape(
            length, rows, chunk
        )

    @pl.loop(0, chunks)
    def _(k):
        sent = outgoing.at[k, pl.ds(0, n - 1)]
        pltpu.make_async_copy(sent, sent, send_sem.at[k]).wait()


def write_kernel(mixed_ref, out_ref, sem):
    copy = pltpu.make_async_copy(mixed_ref, out_ref, sem)
    copy.start()
    copy.wait()


def in_hbm(array):
    return pltpu.with_memory_space_constraint(array, pltpu.HBM)


def local(n, frames, widths, kernel):
    per_device, height, columns = frames.shape
    length = widths.shape[0]
    rows = height // n
    chunk = 256 if columns % 256 == 0 else 128
    chunks = columns // chunk
    hbm = pl.BlockSpec(memory_space=pltpu.HBM)
    vmem = pl.BlockSpec(memory_space=pltpu.VMEM)
    shape = (length, rows, columns)
    mixed = pl.pallas_call(
        functools.partial(exchange_kernel, n),
        out_shape=pltpu.VMEM(shape, jnp.float32),
        in_specs=[hbm] * 3,
        out_specs=vmem,
        scratch_shapes=[
            pltpu.VMEM((per_device, height + 16, columns), jnp.float32),
            pltpu.VMEM((per_device, height // 4 + 16, columns), jnp.float32),
            pltpu.VMEM((chunks, n, per_device * rows, chunk), jnp.float32),
            pltpu.VMEM((chunks, n, per_device * rows, chunk), jnp.float32),
            pltpu.VMEM((length * rows, length * rows), jnp.float32),
            pltpu.VMEM((1, length), jnp.float32),
            pltpu.SMEM((3, 3), jnp.float32),
            pltpu.SemaphoreType.DMA((6,)),
            pltpu.SemaphoreType.DMA((chunks,)),
            pltpu.SemaphoreType.DMA((chunks,)),
            pltpu.SemaphoreType.REGULAR((2,)),
        ],
        compiler_params=pltpu.CompilerParams(
            collective_id=0,
            has_side_effects=True,
            vmem_limit_bytes=50 * 1024 * 1024,
        ),
    )(in_hbm(frames), in_hbm(widths.reshape(1, length)), in_hbm(kernel))
    return pl.pallas_call(
        write_kernel,
        out_shape=pltpu.HBM(shape, jnp.float32),
        in_specs=[vmem],
        out_specs=hbm,
        scratch_shapes=[pltpu.SemaphoreType.DMA],
        compiler_params=pltpu.CompilerParams(vmem_limit_bytes=1024 * 1024),
    )(mixed)


def solution(mesh):
    return jax.shard_map(
        functools.partial(local, mesh.shape["blk"]),
        mesh=mesh,
        in_specs=(P("blk", None, None), P(), P()),
        out_specs=P(None, "blk", None),
        check_vma=False,
    )
```

```python
import functools

import jax
import jax.numpy as jnp
from jax import lax
from jax.experimental import pallas as pl
from jax.experimental.pallas import tpu as pltpu
from jax.sharding import PartitionSpec as P

BAND = 24
LAYERS = 4
MESH = pl.DeviceIdType.MESH


def exchange_kernel(
    n,
    frames_ref,
    widths_hbm,
    kernel_hbm,
    out_ref,
    held,
    window,
    opening,
    outgoing,
    incoming,
    mixing,
    partial,
    widths_ref,
    kernel_ref,
    in_sem,
    send_sem,
    recv_sem,
    round_sem,
):
    per_device, height, columns = frames_ref.shape
    chunks, _, rows_block, chunk = outgoing.shape
    rows = rows_block // per_device
    group = 8 // rows
    length = widths_ref.shape[1]
    me = lax.axis_index("blk")
    quarter = n // LAYERS
    mine = me // quarter
    place = me - mine * quarter
    mirror = 3 - mine
    beside = mine + 1 - 2 * lax.rem(mine, 2)
    across = mirror + 1 - 2 * lax.rem(mirror, 2)
    inner = (mine == 1) | (mine == 2)
    outer = jnp.logical_not(inner)
    front = jnp.where(inner, mirror, beside)
    opposite = mirror * quarter + place
    partner = beside * quarter + place
    part = quarter // group
    seat = place // group
    member_of = place - seat * group
    bits = part.bit_length() - 1
    core_bits = group.bit_length() - 1
    steps = core_bits + bits
    arrived = round_sem.at[2 * steps]
    meet = round_sem.at[2 * steps + 1]
    relay = round_sem.at[2 * steps + 2]

    def flip(value, step):
        return value + step - 2 * step * lax.rem(value // step, 2)

    def mixed_seat(step):
        return lax.rem(seat + step, part)

    strip = height // LAYERS
    first = front * strip

    def load(source, rows_in, target, at, semaphore):
        return pltpu.make_async_copy(
            frames_ref.at[:, pl.ds(pl.multiple_of(source, 8), rows_in), :],
            target.at[:, pl.ds(at, rows_in), :],
            semaphore,
        )

    early = [
        pltpu.make_async_copy(kernel_hbm, kernel_ref, in_sem.at[0]),
        load(first + seat * 8 - 8, 24, opening, 0, in_sem.at[1]),
    ]
    front_load = load(first - 8, strip + 16, window, 0, in_sem.at[2])
    late = [
        load(0, height, held, 8, in_sem.at[3]),
        pltpu.make_async_copy(widths_hbm, widths_ref, in_sem.at[4]),
    ]
    for copy in early:
        copy.start()

    def signal(semaphore, target):
        pl.semaphore_signal(
            semaphore, inc=1, device_id=(target,), device_id_type=MESH
        )

    barrier = pltpu.get_barrier_semaphore()
    neighbours = [flip(place, 1 << bit) for bit in range(core_bits + bits)]
    for place_at in neighbours:
        signal(barrier, mine * quarter + place_at)

    @pl.when(inner)
    def _():
        for layer in (mirror, beside):
            for member in range(group):
                signal(barrier, layer * quarter + seat * group + member)

    edge = jnp.zeros((per_device, 8, columns), jnp.float32)
    held[:, pl.ds(0, 8), :] = edge
    held[:, pl.ds(height + 8, 8), :] = edge
    column = lax.broadcasted_iota(jnp.int32, (8, columns), 1)

    def filter_group(at, source, base):
        for frame in range(per_device):
            start = (at - base) * 8
            if not isinstance(start, int):
                start = pl.multiple_of(start, 8)
            tall = source[frame, pl.ds(start, 24), :]
            taps = [tall[7:15], tall[8:16], tall[9:17]]
            mixed = [
                kernel_ref[0, col] * taps[0]
                + kernel_ref[1, col] * taps[1]
                + kernel_ref[2, col] * taps[2]
                for col in range(3)
            ]
            left = jnp.where(column == 0, 0.0, pltpu.roll(mixed[0], 1, 1))
            right = jnp.where(
                column == columns - 1, 0.0, pltpu.roll(mixed[2], columns - 1, 1)
            )
            value = left + mixed[1] + right
            for member in range(group):
                for k in range(chunks):
                    outgoing[
                        k, at * group + member, pl.ds(frame * rows, rows), :
                    ] = value[
                        member * rows : (member + 1) * rows,
                        k * chunk : (k + 1) * chunk,
                    ]

    def send(k, target):
        pltpu.make_async_remote_copy(
            src_ref=outgoing.at[k, target],
            dst_ref=incoming.at[k, me],
            send_sem=send_sem.at[k],
            recv_sem=recv_sem.at[k, mine],
            device_id=(target,),
            device_id_type=MESH,
        ).start()

    def send_group(at):
        @pl.loop(0, chunks)
        def _(k):
            for member in range(group):
                send(k, at * group + member)

    def send_quarter_at(which, k):
        @pl.loop(0, part)
        def _(step):
            at = which * part + mixed_seat(step)
            for member in range(group):
                send(k, at * group + member)

    def send_quarter(which):
        @pl.loop(0, chunks)
        def _(k):
            send_quarter_at(which, k)

    def send_front_at(k):
        @pl.loop(1, part)
        def _(step):
            at = front * part + mixed_seat(step)
            for member in range(group):
                send(k, at * group + member)

    def send_front(begin, end):
        @pl.loop(begin, end)
        def _(k):
            send_front_at(k)

    def send_near_at(k):
        @pl.loop(1, part)
        def _(step):
            at = mine * part + mixed_seat(step)
            for member in range(group):
                send(k, at * group + member)

        for other in range(1, group):
            send(
                k,
                mine * quarter
                + seat * group
                + lax.rem(member_of + other, group),
            )
        pltpu.make_async_copy(
            outgoing.at[k, me], incoming.at[k, me], recv_sem.at[k, mine]
        ).start()

    def filter_quarter(which):
        @pl.loop(0, part)
        def _(step):
            filter_group(which * part + mixed_seat(step), held, 0)

    for copy in early:
        copy.wait()
    front_load.start()
    for copy in late:
        copy.start()
    own = front * part + seat
    filter_group(own, opening, own)
    pl.semaphore_wait(barrier, group + core_bits + bits)
    send_group(own)

    @pl.when(outer)
    def _():
        signal(arrived, partner)

    def pass_on(bit, at):
        signal(at, mine * quarter + neighbours[bit])

    for bit in range(core_bits):
        pass_on(bit, round_sem.at[bit])
        pl.semaphore_wait(round_sem.at[bit], 1)
    front_load.wait()
    for bit in range(bits):
        at = round_sem.at[core_bits + bit]
        pass_on(core_bits + bit, at)

        @pl.loop(1 << bit, 2 << bit)
        def _(step):
            filter_group(front * part + mixed_seat(step), window, front * part)

        pl.semaphore_wait(at, 1)

    split = jnp.where(inner, min(2, chunks), 0)
    send_front(0, split)
    for copy in late:
        copy.wait()

    @pl.when(inner)
    def _():
        pl.semaphore_wait(arrived, 1)
        for bit in range(steps):
            at = round_sem.at[steps + bit]
            pass_on(bit, at)
            if bit < part:
                filter_group(across * part + mixed_seat(bit), held, 0)
            pl.semaphore_wait(at, 1)
        signal(meet, opposite)

        @pl.loop(min(steps, part), part)
        def _(step):
            filter_group(across * part + mixed_seat(step), held, 0)

        pl.semaphore_wait(meet, 1)
        signal(relay, partner)
        send_quarter(across)

    @pl.when(outer)
    def _():
        filter_quarter(mirror)
        pl.semaphore_wait(relay, 1)
        send_quarter(mirror)

    filter_quarter(mine)

    @pl.when(inner)
    def _():
        filter_quarter(beside)

        @pl.loop(0, chunks)
        def _(k):
            send_quarter_at(beside, k)
            send_near_at(k)

        send_front(split, chunks)

    @pl.when(outer)
    def _():
        @pl.loop(0, chunks)
        def _(k):
            @pl.when(k >= split)
            def _():
                send_front_at(k)
            send_near_at(k)

    @pl.when(outer)
    def _():
        filter_quarter(across)
        send_quarter(across)

    total = length * rows
    target_at = lax.broadcasted_iota(jnp.int32, (total, length), 0) // rows
    lane = lax.broadcasted_iota(jnp.int32, (total, length), 1)
    spread = jnp.sum(
        jnp.where(target_at == lane, widths_ref[...], 0.0), axis=1, keepdims=True
    )
    row_at = lax.broadcasted_iota(jnp.int32, (total, total), 0)
    col_at = lax.broadcasted_iota(jnp.int32, (total, total), 1)
    apart = row_at // rows - col_at // rows
    inside = (jnp.abs(apart) <= BAND) & (row_at % rows == col_at % rows)
    offset = apart.astype(jnp.float32)
    weights = jnp.where(
        inside, jnp.exp(-offset * offset / (2.0 * spread * spread)), 0.0
    )
    weights = weights / jnp.sum(weights, axis=1, keepdims=True)
    depth = total // LAYERS
    high = weights.astype(jnp.bfloat16)
    low = (weights - high.astype(jnp.float32)).astype(jnp.bfloat16)
    for layer in range(LAYERS):
        at = slice(layer * depth, (layer + 1) * depth)
        mixing[layer, :, 0:depth] = high[:, at]
        mixing[layer, :, depth : 2 * depth] = high[:, at]
        mixing[layer, :, 2 * depth : 3 * depth] = low[:, at]

    def share(k, layer):
        block = incoming.at[k, pl.ds(layer * quarter, quarter)]
        pltpu.make_async_copy(block, block, recv_sem.at[k, layer]).wait()
        if rows_block % 8 == 0:
            value = block[...].reshape(depth, chunk)
        else:
            value = jnp.concatenate([block[s] for s in range(quarter)], axis=0)
        value_high = value.astype(jnp.bfloat16)
        value_low = (value - value_high.astype(jnp.float32)).astype(jnp.bfloat16)
        return jnp.dot(
            mixing[layer],
            jnp.concatenate([value_high, value_low, value_high], axis=0),
            preferred_element_type=jnp.float32,
        )

    @pl.loop(0, chunks)
    def _(k):
        partial[...] = share(k, mine)
        partial[...] += share(k, beside)
        partial[...] += share(k, mirror)
        done = partial[...] + share(k, across)
        out_ref[:, :, pl.ds(pl.multiple_of(k * chunk, 128), chunk)] = done.reshape(
            length, rows, chunk
        )

    @pl.loop(0, chunks)
    def _(k):
        sent = outgoing.at[k, pl.ds(0, n - 1)]
        pltpu.make_async_copy(sent, sent, send_sem.at[k]).wait()


def write_kernel(mixed_ref, out_ref, sem):
    copy = pltpu.make_async_copy(mixed_ref, out_ref, sem)
    copy.start()
    copy.wait()


def in_hbm(array):
    return pltpu.with_memory_space_constraint(array, pltpu.HBM)


def local(n, frames, widths, kernel):
    per_device, height, columns = frames.shape
    length = widths.shape[0]
    rows = height // n
    chunk = 256 if columns % 256 == 0 else 128
    chunks = columns // chunk
    total = length * rows
    hbm = pl.BlockSpec(memory_space=pltpu.HBM)
    vmem = pl.BlockSpec(memory_space=pltpu.VMEM)
    shape = (length, rows, columns)
    rounds = 2 * (n // LAYERS).bit_length() + 1
    mixed = pl.pallas_call(
        functools.partial(exchange_kernel, n),
        out_shape=pltpu.VMEM(shape, jnp.float32),
        in_specs=[hbm] * 3,
        out_specs=vmem,
        scratch_shapes=[
            pltpu.VMEM((per_device, height + 16, columns), jnp.float32),
            pltpu.VMEM((per_device, height // LAYERS + 16, columns), jnp.float32),
            pltpu.VMEM((per_device, 24, columns), jnp.float32),
            pltpu.VMEM((chunks, n, per_device * rows, chunk), jnp.float32),
            pltpu.VMEM((chunks, n, per_device * rows, chunk), jnp.float32),
            pltpu.VMEM((LAYERS, total, 3 * total // LAYERS), jnp.bfloat16),
            pltpu.VMEM((total, chunk), jnp.float32),
            pltpu.VMEM((1, length), jnp.float32),
            pltpu.SMEM((3, 3), jnp.float32),
            pltpu.SemaphoreType.DMA((5,)),
            pltpu.SemaphoreType.DMA((chunks,)),
            pltpu.SemaphoreType.DMA((chunks, LAYERS)),
            pltpu.SemaphoreType.REGULAR((rounds,)),
        ],
        compiler_params=pltpu.CompilerParams(
            collective_id=0,
            has_side_effects=True,
            vmem_limit_bytes=50 * 1024 * 1024,
        ),
    )(in_hbm(frames), in_hbm(widths.reshape(1, length)), in_hbm(kernel))
    return pl.pallas_call(
        write_kernel,
        out_shape=pltpu.HBM(shape, jnp.float32),
        in_specs=[vmem],
        out_specs=hbm,
        scratch_shapes=[pltpu.SemaphoreType.DMA],
        compiler_params=pltpu.CompilerParams(vmem_limit_bytes=1024 * 1024),
    )(mixed)


def solution(mesh):
    return jax.shard_map(
        functools.partial(local, mesh.shape["blk"]),
        mesh=mesh,
        in_specs=(P("blk", None, None), P(), P()),
        out_specs=P(None, "blk", None),
        check_vma=False,
    )
```

```python
import functools

import jax
import jax.numpy as jnp
from jax import lax
from jax.experimental import pallas as pl
from jax.experimental.pallas import tpu as pltpu
from jax.sharding import PartitionSpec as P

BAND = 24
LAYERS = 4
MESH = pl.DeviceIdType.MESH


def exchange_kernel(
    n,
    frames_ref,
    widths_hbm,
    kernel_hbm,
    out_ref,
    last_ref,
    rest_ref,
    held,
    window,
    opening,
    outgoing,
    incoming,
    mixing,
    partial,
    widths_ref,
    kernel_ref,
    in_sem,
    send_sem,
    recv_sem,
    round_sem,
):
    per_device, height, columns = frames_ref.shape
    chunks, _, rows_block, chunk = outgoing.shape
    rows = rows_block // per_device
    group = 8 // rows
    length = widths_ref.shape[1]
    me = lax.axis_index("blk")
    quarter = n // LAYERS
    mine = me // quarter
    place = me - mine * quarter
    mirror = 3 - mine
    beside = mine + 1 - 2 * lax.rem(mine, 2)
    across = mirror + 1 - 2 * lax.rem(mirror, 2)
    inner = (mine == 1) | (mine == 2)
    outer = jnp.logical_not(inner)
    front = jnp.where(inner, mirror, beside)
    opposite = mirror * quarter + place
    partner = beside * quarter + place
    part = quarter // group
    seat = place // group
    member_of = place - seat * group
    bits = part.bit_length() - 1
    core_bits = group.bit_length() - 1
    steps = core_bits + bits
    arrived = round_sem.at[2 * steps]
    meet = round_sem.at[2 * steps + 1]
    relay = round_sem.at[2 * steps + 2]

    def flip(value, step):
        return value + step - 2 * step * lax.rem(value // step, 2)

    def mixed_seat(step):
        return lax.rem(seat + step, part)

    def crossed_seat(step):
        total = 0
        for bit in range(bits):
            width = 1 << bit
            total = total + width * lax.rem(seat // width + step // width, 2)
        return total

    own = front * part + seat
    strip = height // LAYERS
    first = front * strip

    def load(source, rows_in, target, at, semaphore):
        return pltpu.make_async_copy(
            frames_ref.at[:, pl.ds(pl.multiple_of(source, 8), rows_in), :],
            target.at[:, pl.ds(at, rows_in), :],
            semaphore,
        )

    taps_load = pltpu.make_async_copy(kernel_hbm, kernel_ref, in_sem.at[0])
    top = pl.multiple_of(first + seat * 8 - 8, 8)
    early = [
        pltpu.make_async_copy(
            frames_ref.at[frame, pl.ds(top, 24), :],
            opening.at[frame],
            in_sem.at[4 + frame],
        )
        for frame in range(per_device)
    ]
    front_load = load(first - 8, strip + 16, window, 0, in_sem.at[1])
    late = [
        load(0, height, held, 8, in_sem.at[2]),
        pltpu.make_async_copy(widths_hbm, widths_ref, in_sem.at[3]),
    ]
    taps_load.start()
    for copy in early:
        copy.start()

    def signal(semaphore, target):
        pl.semaphore_signal(
            semaphore, inc=1, device_id=(target,), device_id_type=MESH
        )

    barrier = pltpu.get_barrier_semaphore()
    neighbours = [flip(place, 1 << bit) for bit in range(core_bits + bits)]
    for place_at in neighbours:
        signal(barrier, mine * quarter + place_at)

    @pl.when(inner)
    def _():
        for layer in (mirror, beside):
            for member in range(group):
                signal(barrier, layer * quarter + seat * group + member)

    edge = jnp.zeros((per_device, 8, columns), jnp.float32)
    held[:, pl.ds(0, 8), :] = edge
    held[:, pl.ds(height + 8, 8), :] = edge
    column = lax.broadcasted_iota(jnp.int32, (8, columns), 1)

    def filter_frame(at, source, frame, start):
        tall = source[frame, pl.ds(start, 24), :]
        taps = [tall[7:15], tall[8:16], tall[9:17]]
        mixed = [
            kernel_ref[0, col] * taps[0]
            + kernel_ref[1, col] * taps[1]
            + kernel_ref[2, col] * taps[2]
            for col in range(3)
        ]
        left = jnp.where(column == 0, 0.0, pltpu.roll(mixed[0], 1, 1))
        right = jnp.where(
            column == columns - 1, 0.0, pltpu.roll(mixed[2], columns - 1, 1)
        )
        value = left + mixed[1] + right
        for member in range(group):
            for k in range(chunks):
                outgoing[
                    k, at * group + member, pl.ds(frame * rows, rows), :
                ] = value[
                    member * rows : (member + 1) * rows,
                    k * chunk : (k + 1) * chunk,
                ]

    def filter_group(at, source, base):
        start = pl.multiple_of((at - base) * 8, 8)
        for frame in range(per_device):
            filter_frame(at, source, frame, start)

    def send(k, target):
        pltpu.make_async_remote_copy(
            src_ref=outgoing.at[k, target],
            dst_ref=incoming.at[k, me],
            send_sem=send_sem.at[k],
            recv_sem=recv_sem.at[k, mine],
            device_id=(target,),
            device_id_type=MESH,
        ).start()

    def send_group(at):
        @pl.loop(0, 4)
        def _(k):
            for member in range(group):
                send(k, at * group + member)

    def send_quarter_at(which, k):
        @pl.loop(0, part)
        def _(step):
            at = which * part + mixed_seat(step)
            for member in range(group):
                send(k, at * group + member)

    def send_quarter(which):
        @pl.loop(0, chunks)
        def _(k):
            send_quarter_at(which, k)

    def send_front_at(k):
        @pl.loop(1, part)
        def _(step):
            at = front * part + mixed_seat(step)
            for member in range(group):
                send(k, at * group + member)

        @pl.when(outer | (k >= 4))
        def _():
            for member in range(group):
                send(k, own * group + member)

    def send_front(begin, end):
        @pl.loop(begin, end)
        def _(k):
            send_front_at(k)

    def send_near_at(k):
        @pl.loop(1, part)
        def _(step):
            at = mine * part + mixed_seat(step)
            for member in range(group):
                send(k, at * group + member)

        for other in range(1, group):
            send(
                k,
                mine * quarter
                + seat * group
                + lax.rem(member_of + other, group),
            )
        pltpu.make_async_copy(
            outgoing.at[k, me], incoming.at[k, me], recv_sem.at[k, mine]
        ).start()

    def filter_quarter(which):
        @pl.loop(0, part)
        def _(step):
            filter_group(which * part + mixed_seat(step), held, 0)

    taps_load.wait()
    for frame in range(per_device):
        early[frame].wait()
        filter_frame(own, opening, frame, 0)
    front_load.start()
    for copy in late:
        copy.start()
    pl.semaphore_wait(barrier, group + core_bits + bits)
    pl.when(inner)(lambda: send_group(own))

    @pl.when(outer)
    def _():
        signal(arrived, partner)

    def pass_on(bit, at):
        signal(at, mine * quarter + neighbours[bit])

    for bit in range(core_bits):
        pass_on(bit, round_sem.at[bit])
        pl.semaphore_wait(round_sem.at[bit], 1)
    front_load.wait()
    for bit in range(bits):
        at = round_sem.at[core_bits + bit]
        pass_on(core_bits + bit, at)

        @pl.loop(1 << bit, 2 << bit)
        def _(step):
            filter_group(front * part + crossed_seat(step), window, front * part)

        pl.semaphore_wait(at, 1)

        @pl.when(inner)
        def _():
            @pl.loop(1 << bit, 2 << bit)
            def _(step):
                for member in range(group):
                    send(0, (front * part + crossed_seat(step)) * group + member)

    split = jnp.where(inner, min(2, chunks), 0)
    send_front(1, split)
    for copy in late:
        copy.wait()

    @pl.when(inner)
    def _():
        pl.semaphore_wait(arrived, 1)
        for bit in range(steps):
            at = round_sem.at[steps + bit]
            pass_on(bit, at)
            if bit < part:
                filter_group(across * part + mixed_seat(bit), held, 0)
            pl.semaphore_wait(at, 1)
        signal(meet, opposite)

        @pl.loop(min(steps, part), part)
        def _(step):
            filter_group(across * part + mixed_seat(step), held, 0)

        pl.semaphore_wait(meet, 1)
        signal(relay, partner)
        send_quarter(across)

    filter_quarter(mine)

    @pl.when(inner)
    def _():
        filter_quarter(beside)

        @pl.loop(0, chunks)
        def _(k):
            send_quarter_at(beside, k)
            send_near_at(k)

        send_front(split, chunks)

    @pl.when(outer)
    def _():
        filter_quarter(mirror)
        pl.semaphore_wait(relay, 1)

        @pl.loop(0, chunks)
        def _(k):
            send_quarter_at(mirror, k)
            send_front_at(k)
            send_near_at(k)

    @pl.when(outer)
    def _():
        filter_quarter(across)
        send_quarter(across)

    total = length * rows
    target_at = lax.broadcasted_iota(jnp.int32, (total, length), 0) // rows
    lane = lax.broadcasted_iota(jnp.int32, (total, length), 1)
    spread = jnp.sum(
        jnp.where(target_at == lane, widths_ref[...], 0.0), axis=1, keepdims=True
    )
    row_at = lax.broadcasted_iota(jnp.int32, (total, total), 0)
    col_at = lax.broadcasted_iota(jnp.int32, (total, total), 1)
    apart = row_at // rows - col_at // rows
    inside = (jnp.abs(apart) <= BAND) & (row_at % rows == col_at % rows)
    offset = apart.astype(jnp.float32)
    weights = jnp.where(
        inside, jnp.exp(-offset * offset / (2.0 * spread * spread)), 0.0
    )
    weights = weights / jnp.sum(weights, axis=1, keepdims=True)
    depth = total // LAYERS
    high = weights.astype(jnp.bfloat16)
    low = (weights - high.astype(jnp.float32)).astype(jnp.bfloat16)
    for layer in range(LAYERS):
        at = slice(layer * depth, (layer + 1) * depth)
        mixing[layer, :, 0:depth] = high[:, at]
        mixing[layer, :, depth : 2 * depth] = high[:, at]
        mixing[layer, :, 2 * depth : 3 * depth] = low[:, at]

    last_ref[...] = mixing[mirror]

    def arrive(k, layer):
        block = incoming.at[k, pl.ds(layer * quarter, quarter)]
        pltpu.make_async_copy(block, block, recv_sem.at[k, layer]).wait()
        return block

    def share(k, layer):
        block = arrive(k, layer)
        if rows_block % 8 == 0:
            value = block[...].reshape(depth, chunk)
        else:
            value = jnp.concatenate([block[s] for s in range(quarter)], axis=0)
        return product(mixing[layer], value)

    def put(k, value):
        out_ref[:, :, pl.ds(pl.multiple_of(k * chunk, 128), chunk)] = value.reshape(
            length, rows, chunk
        )

    @pl.loop(0, chunks)
    def _(k):
        partial[...] = share(k, mine)
        partial[...] += share(k, beside)

        @pl.when(k < chunks - 1)
        def _():
            partial[...] += share(k, across)
            put(k, partial[...] + share(k, mirror))

        @pl.when(k == chunks - 1)
        def _():
            put(k, partial[...] + share(k, across))

    block = arrive(chunks - 1, mirror)
    if rows_block % 8 == 0:
        value = block[...].reshape(depth, chunk)
    else:
        value = jnp.concatenate([block[s] for s in range(quarter)], axis=0)
    rest_ref[...] = value

    @pl.loop(0, chunks)
    def _(k):
        sent = outgoing.at[k, pl.ds(0, n - 1)]
        pltpu.make_async_copy(sent, sent, send_sem.at[k]).wait()


def product(weights, value):
    high = value.astype(jnp.bfloat16)
    low = (value - high.astype(jnp.float32)).astype(jnp.bfloat16)
    return jnp.dot(
        weights,
        jnp.concatenate([high, low, high], axis=0),
        preferred_element_type=jnp.float32,
    )


def write_kernel(mixed_ref, last_ref, rest_ref, out_ref, end, sem):
    length, rows, columns = mixed_ref.shape
    chunk = rest_ref.shape[1]
    begin = columns - chunk
    ready = pltpu.make_async_copy(
        mixed_ref.at[:, :, pl.ds(0, begin)],
        out_ref.at[:, :, pl.ds(0, begin)],
        sem.at[0],
    )
    ready.start()
    end[...] = mixed_ref[:, :, begin:] + product(
        last_ref[...], rest_ref[...]
    ).reshape(length, rows, chunk)
    final = pltpu.make_async_copy(end, out_ref.at[:, :, pl.ds(begin, chunk)], sem.at[1])
    final.start()
    ready.wait()
    final.wait()


def in_hbm(array):
    return pltpu.with_memory_space_constraint(array, pltpu.HBM)


def local(n, frames, widths, kernel):
    per_device, height, columns = frames.shape
    length = widths.shape[0]
    rows = height // n
    chunk = 256 if columns % 256 == 0 else 128
    chunks = columns // chunk
    total = length * rows
    depth = total // LAYERS
    hbm = pl.BlockSpec(memory_space=pltpu.HBM)
    vmem = pl.BlockSpec(memory_space=pltpu.VMEM)
    shape = (length, rows, columns)
    rounds = 2 * (n // LAYERS).bit_length() + 1
    mixed = pl.pallas_call(
        functools.partial(exchange_kernel, n),
        out_shape=(
            pltpu.VMEM(shape, jnp.float32),
            pltpu.VMEM((total, 3 * depth), jnp.bfloat16),
            pltpu.VMEM((depth, chunk), jnp.float32),
        ),
        in_specs=[hbm] * 3,
        out_specs=(vmem, vmem, vmem),
        scratch_shapes=[
            pltpu.VMEM((per_device, height + 16, columns), jnp.float32),
            pltpu.VMEM((per_device, height // LAYERS + 16, columns), jnp.float32),
            pltpu.VMEM((per_device, 24, columns), jnp.float32),
            pltpu.VMEM((chunks, n, per_device * rows, chunk), jnp.float32),
            pltpu.VMEM((chunks, n, per_device * rows, chunk), jnp.float32),
            pltpu.VMEM((LAYERS, total, 3 * total // LAYERS), jnp.bfloat16),
            pltpu.VMEM((total, chunk), jnp.float32),
            pltpu.VMEM((1, length), jnp.float32),
            pltpu.SMEM((3, 3), jnp.float32),
            pltpu.SemaphoreType.DMA((4 + per_device,)),
            pltpu.SemaphoreType.DMA((chunks,)),
            pltpu.SemaphoreType.DMA((chunks, LAYERS)),
            pltpu.SemaphoreType.REGULAR((rounds,)),
        ],
        compiler_params=pltpu.CompilerParams(
            collective_id=0,
            has_side_effects=True,
            vmem_limit_bytes=50 * 1024 * 1024,
        ),
    )(in_hbm(frames), in_hbm(widths.reshape(1, length)), in_hbm(kernel))
    return pl.pallas_call(
        write_kernel,
        out_shape=pltpu.HBM(shape, jnp.float32),
        in_specs=[vmem] * 3,
        out_specs=hbm,
        scratch_shapes=[
            pltpu.VMEM((length, rows, chunk), jnp.float32),
            pltpu.SemaphoreType.DMA((2,)),
        ],
        compiler_params=pltpu.CompilerParams(vmem_limit_bytes=4 * 1024 * 1024),
    )(*mixed)


def solution(mesh):
    return jax.shard_map(
        functools.partial(local, mesh.shape["blk"]),
        mesh=mesh,
        in_specs=(P("blk", None, None), P(), P()),
        out_specs=P(None, "blk", None),
        check_vma=False,
    )
```

```python
import functools

import jax
import jax.numpy as jnp
from jax import lax
from jax.experimental import pallas as pl
from jax.experimental.pallas import tpu as pltpu
from jax.sharding import PartitionSpec as P

BAND = 24
LAYERS = 4
MESH = pl.DeviceIdType.MESH


def exchange_kernel(
    n,
    frames_ref,
    widths_hbm,
    kernel_hbm,
    out_ref,
    last_ref,
    rest_ref,
    held,
    window,
    opening,
    outgoing,
    incoming,
    mixing,
    partial,
    widths_ref,
    kernel_ref,
    in_sem,
    send_sem,
    recv_sem,
    round_sem,
):
    per_device, height, columns = frames_ref.shape
    chunks, _, rows_block, chunk = outgoing.shape
    rows = rows_block // per_device
    group = 8 // rows
    held_back = max(chunks - 1, 1)
    length = widths_ref.shape[1]
    me = lax.axis_index("blk")
    quarter = n // LAYERS
    mine = me // quarter
    place = me - mine * quarter
    mirror = 3 - mine
    beside = mine + 1 - 2 * lax.rem(mine, 2)
    across = mirror + 1 - 2 * lax.rem(mirror, 2)
    inner = (mine == 1) | (mine == 2)
    outer = jnp.logical_not(inner)
    front = jnp.where(inner, mirror, beside)
    opposite = mirror * quarter + place
    partner = beside * quarter + place
    part = quarter // group
    seat = place // group
    member_of = place - seat * group
    bits = part.bit_length() - 1
    core_bits = group.bit_length() - 1
    steps = core_bits + bits
    arrived = round_sem.at[2 * steps]
    meet = round_sem.at[2 * steps + 1]
    relay = round_sem.at[2 * steps + 2]

    def flip(value, step):
        return value + step - 2 * step * lax.rem(value // step, 2)

    def mixed_seat(step):
        return lax.rem(seat + step, part)

    def crossed_seat(step):
        total = 0
        for bit in range(bits):
            width = 1 << bit
            total = total + width * lax.rem(seat // width + step // width, 2)
        return total

    own = front * part + seat
    strip = height // LAYERS
    first = front * strip

    def load(source, rows_in, target, at, semaphore):
        return pltpu.make_async_copy(
            frames_ref.at[:, pl.ds(pl.multiple_of(source, 8), rows_in), :],
            target.at[:, pl.ds(at, rows_in), :],
            semaphore,
        )

    taps_load = pltpu.make_async_copy(kernel_hbm, kernel_ref, in_sem.at[0])
    top = pl.multiple_of(first + seat * 8 - 8, 8)
    margin = min(chunk + 128, columns)
    edges = [(0, margin)] + ([(margin, columns)] if margin < columns else [])
    early = [
        pltpu.make_async_copy(
            frames_ref.at[:, pl.ds(top, 24), pl.ds(begin, end - begin)],
            opening.at[:, :, pl.ds(begin, end - begin)],
            in_sem.at[4 + at],
        )
        for at, (begin, end) in enumerate(edges)
    ]
    front_load = load(first - 8, strip + 16, window, 0, in_sem.at[1])
    late = [
        load(0, height, held, 8, in_sem.at[2]),
        pltpu.make_async_copy(widths_hbm, widths_ref, in_sem.at[3]),
    ]
    taps_load.start()
    for copy in early:
        copy.start()
    front_load.start()

    def signal(semaphore, target):
        pl.semaphore_signal(
            semaphore, inc=1, device_id=(target,), device_id_type=MESH
        )

    barrier = pltpu.get_barrier_semaphore()
    neighbours = [flip(place, 1 << bit) for bit in range(core_bits + bits)]
    for place_at in neighbours:
        signal(barrier, mine * quarter + place_at)

    @pl.when(inner)
    def _():
        for layer in (mirror, beside):
            for member in range(group):
                signal(barrier, layer * quarter + seat * group + member)

    edge = jnp.zeros((per_device, 8, columns), jnp.float32)
    held[:, pl.ds(0, 8), :] = edge
    held[:, pl.ds(height + 8, 8), :] = edge

    def filter_frame(at, source, frame, start, begin=0, end=None):
        end = columns if end is None else end
        low, high = max(begin - 128, 0), min(end + 128, columns)
        wide = high - low
        tall = source[frame, pl.ds(start, 24), low:high]
        taps = [tall[7:15], tall[8:16], tall[9:17]]
        mixed = [
            kernel_ref[0, col] * taps[0]
            + kernel_ref[1, col] * taps[1]
            + kernel_ref[2, col] * taps[2]
            for col in range(3)
        ]
        left = pltpu.roll(mixed[0], 1, 1)
        right = pltpu.roll(mixed[2], wide - 1, 1)
        lane = lax.broadcasted_iota(jnp.int32, (8, wide), 1) + low
        if low == 0:
            left = jnp.where(lane == 0, 0.0, left)
        if high == columns:
            right = jnp.where(lane == columns - 1, 0.0, right)
        value = left + mixed[1] + right
        for member in range(group):
            for k in range(begin // chunk, end // chunk):
                outgoing[
                    k, at * group + member, pl.ds(frame * rows, rows), :
                ] = value[
                    member * rows : (member + 1) * rows,
                    k * chunk - low : (k + 1) * chunk - low,
                ]

    def filter_group(at, source, base):
        start = pl.multiple_of((at - base) * 8, 8)
        for frame in range(per_device):
            filter_frame(at, source, frame, start)

    def send(k, target):
        pltpu.make_async_remote_copy(
            src_ref=outgoing.at[k, target],
            dst_ref=incoming.at[k, me],
            send_sem=send_sem.at[k],
            recv_sem=recv_sem.at[k, mine],
            device_id=(target,),
            device_id_type=MESH,
        ).start()

    def send_group(at):
        @pl.loop(1, held_back)
        def _(k):
            for member in range(group):
                send(k, at * group + member)

    def send_quarter_at(which, k):
        @pl.loop(0, part)
        def _(step):
            at = which * part + lax.rem(seat + part + step * (1 - 2 * lax.rem(me, 2)), part)
            for member in range(group):
                send(k, at * group + member)

    def send_quarter(which):
        @pl.loop(0, chunks)
        def _(k):
            send_quarter_at(which, k)

    def send_front_at(k):
        @pl.loop(1, part)
        def _(step):
            at = front * part + mixed_seat(step)
            for member in range(group):
                send(k, at * group + member)

        @pl.when(outer | (k >= held_back))
        def _():
            for member in range(group):
                send(k, own * group + member)

    def send_front(begin, end):
        @pl.loop(begin, end)
        def _(k):
            send_front_at(k)

    def send_near_at(k):
        @pl.loop(1, part)
        def _(step):
            at = mine * part + mixed_seat(step)
            for member in range(group):
                send(k, at * group + member)

        for other in range(1, group):
            send(
                k,
                mine * quarter
                + seat * group
                + lax.rem(member_of + other, group),
            )
        pltpu.make_async_copy(
            outgoing.at[k, me], incoming.at[k, me], recv_sem.at[k, mine]
        ).start()

    def filter_quarter(which):
        @pl.loop(0, part)
        def _(step):
            filter_group(which * part + mixed_seat(step), held, 0)

    taps_load.wait()
    early[0].wait()
    for frame in range(per_device):
        filter_frame(own, opening, frame, 0, 0, chunk)
    pl.semaphore_wait(barrier, group + steps)

    @pl.when(inner)
    def _():
        for member in range(group):
            send(0, own * group + member)

    if chunks > 1:
        early[-1].wait()
        for frame in range(per_device):
            filter_frame(own, opening, frame, 0, chunk, columns)
        pl.when(inner)(lambda: send_group(own))
    for copy in late:
        copy.start()

    @pl.when(outer)
    def _():
        signal(arrived, partner)

    def pass_on(bit, at):
        signal(at, mine * quarter + neighbours[bit])

    for bit in range(core_bits):
        pass_on(bit, round_sem.at[bit])
        pl.semaphore_wait(round_sem.at[bit], 1)
    for bit in range(bits):
        at = round_sem.at[core_bits + bit]
        pass_on(core_bits + bit, at)
        if bit == 0:
            front_load.wait()

        @pl.loop(1 << bit, 2 << bit)
        def _(step):
            filter_group(front * part + crossed_seat(step), window, front * part)

        pl.semaphore_wait(at, 1)

        @pl.when(inner)
        def _():
            @pl.loop(1 << bit, 2 << bit)
            def _(step):
                for member in range(group):
                    send(0, (front * part + crossed_seat(step)) * group + member)

    split = jnp.where(inner, min(2, chunks), 0)
    send_front(1, split)
    for copy in late:
        copy.wait()

    @pl.when(inner)
    def _():
        pl.semaphore_wait(arrived, 1)
        for bit in range(steps):
            at = round_sem.at[steps + bit]
            pass_on(bit, at)
            if bit < part:
                filter_group(across * part + mixed_seat(bit), held, 0)
            pl.semaphore_wait(at, 1)
        signal(meet, opposite)

        @pl.loop(min(steps, part), part)
        def _(step):
            filter_group(across * part + mixed_seat(step), held, 0)

        pl.semaphore_wait(meet, 1)
        signal(relay, partner)
        filter_quarter(mine)
        send_quarter(across)

    pl.when(outer)(lambda: filter_quarter(mine))

    @pl.when(inner)
    def _():
        filter_quarter(beside)

        @pl.loop(0, chunks)
        def _(k):
            send_quarter_at(beside, k)
            send_near_at(k)

        send_front(split, chunks)

    @pl.when(outer)
    def _():
        filter_quarter(mirror)
        pl.semaphore_wait(relay, 1)

        @pl.loop(0, chunks)
        def _(k):
            send_quarter_at(mirror, k)
            send_front_at(k)
            send_near_at(k)

    @pl.when(outer)
    def _():
        filter_quarter(across)
        send_quarter(across)

    total = length * rows
    target_at = lax.broadcasted_iota(jnp.int32, (total, length), 0) // rows
    lane = lax.broadcasted_iota(jnp.int32, (total, length), 1)
    spread = jnp.sum(
        jnp.where(target_at == lane, widths_ref[...], 0.0), axis=1, keepdims=True
    )
    row_at = lax.broadcasted_iota(jnp.int32, (total, total), 0)
    col_at = lax.broadcasted_iota(jnp.int32, (total, total), 1)
    apart = row_at // rows - col_at // rows
    inside = (jnp.abs(apart) <= BAND) & (row_at % rows == col_at % rows)
    offset = apart.astype(jnp.float32)
    weights = jnp.where(
        inside, jnp.exp(-offset * offset / (2.0 * spread * spread)), 0.0
    )
    weights = weights / jnp.sum(weights, axis=1, keepdims=True)
    depth = total // LAYERS
    high = weights.astype(jnp.bfloat16)
    low = (weights - high.astype(jnp.float32)).astype(jnp.bfloat16)
    for layer in range(LAYERS):
        at = slice(layer * depth, (layer + 1) * depth)
        mixing[layer, :, 0:depth] = high[:, at]
        mixing[layer, :, depth : 2 * depth] = high[:, at]
        mixing[layer, :, 2 * depth : 3 * depth] = low[:, at]

    last_ref[...] = mixing[mirror]

    def arrive(k, layer):
        block = incoming.at[k, pl.ds(layer * quarter, quarter)]
        pltpu.make_async_copy(block, block, recv_sem.at[k, layer]).wait()
        return block

    def share(k, layer):
        block = arrive(k, layer)
        if rows_block % 8 == 0:
            value = block[...].reshape(depth, chunk)
        else:
            value = jnp.concatenate([block[s] for s in range(quarter)], axis=0)
        return product(mixing[layer], value)

    def put(k, value):
        out_ref[:, :, pl.ds(pl.multiple_of(k * chunk, 128), chunk)] = value.reshape(
            length, rows, chunk
        )

    @pl.loop(0, chunks)
    def _(k):
        partial[...] = share(k, mine)
        partial[...] += share(k, beside)

        @pl.when(k < chunks - 1)
        def _():
            partial[...] += share(k, across)
            put(k, partial[...] + share(k, mirror))

        @pl.when(k == chunks - 1)
        def _():
            put(k, partial[...] + share(k, across))

    block = arrive(chunks - 1, mirror)
    if rows_block % 8 == 0:
        value = block[...].reshape(depth, chunk)
    else:
        value = jnp.concatenate([block[s] for s in range(quarter)], axis=0)
    rest_ref[...] = value

    @pl.loop(0, chunks)
    def _(k):
        sent = outgoing.at[k, pl.ds(0, n - 1)]
        pltpu.make_async_copy(sent, sent, send_sem.at[k]).wait()


def product(weights, value):
    high = value.astype(jnp.bfloat16)
    low = (value - high.astype(jnp.float32)).astype(jnp.bfloat16)
    return jnp.dot(
        weights,
        jnp.concatenate([high, low, high], axis=0),
        preferred_element_type=jnp.float32,
    )


def write_kernel(mixed_ref, last_ref, rest_ref, out_ref, end, sem):
    length, rows, columns = mixed_ref.shape
    chunk = rest_ref.shape[1]
    begin = columns - chunk
    ready = pltpu.make_async_copy(
        mixed_ref.at[:, :, pl.ds(0, begin)],
        out_ref.at[:, :, pl.ds(0, begin)],
        sem.at[0],
    )
    ready.start()
    end[...] = mixed_ref[:, :, begin:] + product(
        last_ref[...], rest_ref[...]
    ).reshape(length, rows, chunk)
    final = pltpu.make_async_copy(end, out_ref.at[:, :, pl.ds(begin, chunk)], sem.at[1])
    final.start()
    ready.wait()
    final.wait()


def in_hbm(array):
    return pltpu.with_memory_space_constraint(array, pltpu.HBM)


def local(n, frames, widths, kernel):
    per_device, height, columns = frames.shape
    length = widths.shape[0]
    rows = height // n
    chunk = 256 if columns % 256 == 0 else 128
    chunks = columns // chunk
    total = length * rows
    depth = total // LAYERS
    hbm = pl.BlockSpec(memory_space=pltpu.HBM)
    vmem = pl.BlockSpec(memory_space=pltpu.VMEM)
    shape = (length, rows, columns)
    rounds = 2 * (n // LAYERS).bit_length() + 1
    mixed = pl.pallas_call(
        functools.partial(exchange_kernel, n),
        out_shape=(
            pltpu.VMEM(shape, jnp.float32),
            pltpu.VMEM((total, 3 * depth), jnp.bfloat16),
            pltpu.VMEM((depth, chunk), jnp.float32),
        ),
        in_specs=[hbm] * 3,
        out_specs=(vmem, vmem, vmem),
        scratch_shapes=[
            pltpu.VMEM((per_device, height + 16, columns), jnp.float32),
            pltpu.VMEM((per_device, height // LAYERS + 16, columns), jnp.float32),
            pltpu.VMEM((per_device, 24, columns), jnp.float32),
            pltpu.VMEM((chunks, n, per_device * rows, chunk), jnp.float32),
            pltpu.VMEM((chunks, n, per_device * rows, chunk), jnp.float32),
            pltpu.VMEM((LAYERS, total, 3 * total // LAYERS), jnp.bfloat16),
            pltpu.VMEM((total, chunk), jnp.float32),
            pltpu.VMEM((1, length), jnp.float32),
            pltpu.SMEM((3, 3), jnp.float32),
            pltpu.SemaphoreType.DMA((6,)),
            pltpu.SemaphoreType.DMA((chunks,)),
            pltpu.SemaphoreType.DMA((chunks, LAYERS)),
            pltpu.SemaphoreType.REGULAR((rounds,)),
        ],
        compiler_params=pltpu.CompilerParams(
            collective_id=0,
            has_side_effects=True,
            vmem_limit_bytes=50 * 1024 * 1024,
        ),
    )(in_hbm(frames), in_hbm(widths.reshape(1, length)), in_hbm(kernel))
    return pl.pallas_call(
        write_kernel,
        out_shape=pltpu.HBM(shape, jnp.float32),
        in_specs=[vmem] * 3,
        out_specs=hbm,
        scratch_shapes=[
            pltpu.VMEM((length, rows, chunk), jnp.float32),
            pltpu.SemaphoreType.DMA((2,)),
        ],
        compiler_params=pltpu.CompilerParams(vmem_limit_bytes=4 * 1024 * 1024),
    )(*mixed)


def solution(mesh):
    return jax.shard_map(
        functools.partial(local, mesh.shape["blk"]),
        mesh=mesh,
        in_specs=(P("blk", None, None), P(), P()),
        out_specs=P(None, "blk", None),
        check_vma=False,
    )
```

```python
import functools

import jax
import jax.numpy as jnp
from jax import lax
from jax.experimental import pallas as pl
from jax.experimental.pallas import tpu as pltpu
from jax.sharding import PartitionSpec as P

BAND = 24
LAYERS = 4
MESH = pl.DeviceIdType.MESH


def exchange_kernel(
    n,
    frames_ref,
    widths_hbm,
    kernel_hbm,
    out_ref,
    last_ref,
    rest_ref,
    held,
    window,
    opening,
    outgoing,
    incoming,
    mixing,
    partial,
    widths_ref,
    kernel_ref,
    in_sem,
    send_sem,
    recv_sem,
    round_sem,
):
    per_device, height, columns = frames_ref.shape
    chunks, _, rows_block, chunk = outgoing.shape
    rows = rows_block // per_device
    group = 8 // rows
    held_back = max(chunks - 1, 1)
    length = widths_ref.shape[1]
    me = lax.axis_index("blk")
    quarter = n // LAYERS
    mine = me // quarter
    place = me - mine * quarter
    mirror = 3 - mine
    beside = mine + 1 - 2 * lax.rem(mine, 2)
    across = mirror + 1 - 2 * lax.rem(mirror, 2)
    inner = (mine == 1) | (mine == 2)
    outer = jnp.logical_not(inner)
    front = jnp.where(inner, mirror, beside)
    opposite = mirror * quarter + place
    partner = beside * quarter + place
    part = quarter // group
    seat = place // group
    member_of = place - seat * group
    bits = part.bit_length() - 1
    core_bits = group.bit_length() - 1
    steps = core_bits + bits
    arrived = round_sem.at[2 * steps]
    meet = round_sem.at[2 * steps + 1]
    relay = round_sem.at[2 * steps + 2]

    def flip(value, step):
        return value + step - 2 * step * lax.rem(value // step, 2)

    def mixed_seat(step):
        return lax.rem(seat + step, part)

    def crossed_seat(step):
        total = 0
        for bit in range(bits):
            width = 1 << bit
            total = total + width * lax.rem(seat // width + step // width, 2)
        return total

    own = front * part + seat
    strip = height // LAYERS
    first = front * strip

    def load(source, rows_in, target, at, semaphore):
        return pltpu.make_async_copy(
            frames_ref.at[:, pl.ds(pl.multiple_of(source, 8), rows_in), :],
            target.at[:, pl.ds(at, rows_in), :],
            semaphore,
        )

    taps_load = pltpu.make_async_copy(kernel_hbm, kernel_ref, in_sem.at[0])
    top = pl.multiple_of(first + seat * 8 - 8, 8)
    margin = min(chunk + 128, columns)
    edges = [(0, margin)] + ([(margin, columns)] if margin < columns else [])
    early = [
        pltpu.make_async_copy(
            frames_ref.at[:, pl.ds(top, 24), pl.ds(begin, end - begin)],
            opening.at[:, :, pl.ds(begin, end - begin)],
            in_sem.at[4 + at],
        )
        for at, (begin, end) in enumerate(edges)
    ]
    front_load = load(first - 8, strip + 16, window, 0, in_sem.at[1])
    late = [
        load(0, height, held, 8, in_sem.at[2]),
        pltpu.make_async_copy(widths_hbm, widths_ref, in_sem.at[3]),
    ]
    taps_load.start()
    for copy in early:
        copy.start()
    front_load.start()

    def signal(semaphore, target):
        pl.semaphore_signal(
            semaphore, inc=1, device_id=(target,), device_id_type=MESH
        )

    barrier = pltpu.get_barrier_semaphore()
    neighbours = [flip(place, 1 << bit) for bit in range(core_bits + bits)]
    for place_at in neighbours:
        signal(barrier, mine * quarter + place_at)

    @pl.when(inner)
    def _():
        for layer in (mirror, beside):
            for member in range(group):
                signal(barrier, layer * quarter + seat * group + member)

    edge = jnp.zeros((per_device, 8, columns), jnp.float32)
    held[:, pl.ds(0, 8), :] = edge
    held[:, pl.ds(height + 8, 8), :] = edge

    def filter_frame(at, source, frame, start, begin=0, end=None):
        end = columns if end is None else end
        low, high = max(begin - 128, 0), min(end + 128, columns)
        wide = high - low
        tall = source[frame, pl.ds(start, 24), low:high]
        taps = [tall[7:15], tall[8:16], tall[9:17]]
        mixed = [
            kernel_ref[0, col] * taps[0]
            + kernel_ref[1, col] * taps[1]
            + kernel_ref[2, col] * taps[2]
            for col in range(3)
        ]
        left = pltpu.roll(mixed[0], 1, 1)
        right = pltpu.roll(mixed[2], wide - 1, 1)
        lane = lax.broadcasted_iota(jnp.int32, (8, wide), 1) + low
        if low == 0:
            left = jnp.where(lane == 0, 0.0, left)
        if high == columns:
            right = jnp.where(lane == columns - 1, 0.0, right)
        value = left + mixed[1] + right
        for member in range(group):
            for k in range(begin // chunk, end // chunk):
                outgoing[
                    k, at * group + member, pl.ds(frame * rows, rows), :
                ] = value[
                    member * rows : (member + 1) * rows,
                    k * chunk - low : (k + 1) * chunk - low,
                ]

    def filter_group(at, source, base):
        start = pl.multiple_of((at - base) * 8, 8)
        for frame in range(per_device):
            filter_frame(at, source, frame, start)

    def send(k, target):
        pltpu.make_async_remote_copy(
            src_ref=outgoing.at[k, target],
            dst_ref=incoming.at[k, me],
            send_sem=send_sem.at[k],
            recv_sem=recv_sem.at[k, mine],
            device_id=(target,),
            device_id_type=MESH,
        ).start()

    def send_group(at):
        @pl.loop(1, held_back)
        def _(k):
            for member in range(group):
                send(k, at * group + member)

    def send_quarter_at(which, k):
        @pl.loop(0, part)
        def _(step):
            at = which * part + lax.rem(seat + part + step * (1 - 2 * lax.rem(me, 2)), part)
            for member in range(group):
                send(k, at * group + member)

    def send_quarter(which):
        @pl.loop(0, chunks)
        def _(k):
            send_quarter_at(which, k)

    def send_front_at(k):
        @pl.loop(1, part)
        def _(step):
            seat_at = jnp.where(
                k >= held_back, crossed_seat(part - step), mixed_seat(step)
            )
            at = front * part + seat_at
            for member in range(group):
                send(k, at * group + member)

        @pl.when(outer | (k >= held_back))
        def _():
            for member in reversed(range(group)):
                send(k, own * group + member)

    def send_front(begin, end):
        @pl.loop(begin, end)
        def _(k):
            send_front_at(k)

    def send_near_at(k):
        @pl.loop(1, part)
        def _(step):
            at = mine * part + mixed_seat(step)
            for member in range(group):
                send(k, at * group + member)

        for other in range(1, group):
            send(
                k,
                mine * quarter
                + seat * group
                + lax.rem(member_of + other, group),
            )
        pltpu.make_async_copy(
            outgoing.at[k, me], incoming.at[k, me], recv_sem.at[k, mine]
        ).start()

    def filter_quarter(which):
        @pl.loop(0, part)
        def _(step):
            filter_group(which * part + mixed_seat(step), held, 0)

    taps_load.wait()
    early[0].wait()
    for frame in range(per_device):
        filter_frame(own, opening, frame, 0, 0, chunk)
    pl.semaphore_wait(barrier, group + steps)

    @pl.when(inner)
    def _():
        for member in range(group):
            send(0, own * group + member)

    if chunks > 1:
        early[-1].wait()
        for frame in range(per_device):
            filter_frame(own, opening, frame, 0, chunk, columns)
        pl.when(inner)(lambda: send_group(own))
    for copy in late:
        copy.start()

    @pl.when(outer)
    def _():
        signal(arrived, partner)

    def pass_on(bit, at):
        signal(at, mine * quarter + neighbours[bit])

    for bit in range(core_bits):
        pass_on(bit, round_sem.at[bit])
        pl.semaphore_wait(round_sem.at[bit], 1)
    for bit in range(bits):
        at = round_sem.at[core_bits + bit]
        pass_on(core_bits + bit, at)
        if bit == 0:
            front_load.wait()

        @pl.loop(1 << bit, 2 << bit)
        def _(step):
            filter_group(front * part + crossed_seat(step), window, front * part)

        pl.semaphore_wait(at, 1)

        @pl.when(inner)
        def _():
            @pl.loop(1 << bit, 2 << bit)
            def _(step):
                for member in range(group):
                    send(0, (front * part + crossed_seat(step)) * group + member)

    split = jnp.where(inner, min(2, chunks), 0)
    send_front(1, split)
    for copy in late:
        copy.wait()

    @pl.when(inner)
    def _():
        pl.semaphore_wait(arrived, 1)
        for bit in range(steps):
            at = round_sem.at[steps + bit]
            pass_on(bit, at)
            if bit < part:
                filter_group(across * part + mixed_seat(bit), held, 0)
            pl.semaphore_wait(at, 1)
        signal(meet, opposite)

        @pl.loop(min(steps, part), part)
        def _(step):
            filter_group(across * part + mixed_seat(step), held, 0)

        pl.semaphore_wait(meet, 1)
        signal(relay, partner)
        filter_quarter(mine)
        send_quarter(across)

    pl.when(outer)(lambda: filter_quarter(mine))

    @pl.when(inner)
    def _():
        filter_quarter(beside)

        @pl.loop(0, chunks)
        def _(k):
            send_quarter_at(beside, k)
            send_near_at(k)

        send_front(split, chunks)

    @pl.when(outer)
    def _():
        filter_quarter(mirror)
        pl.semaphore_wait(relay, 1)

        @pl.loop(0, chunks)
        def _(k):
            send_quarter_at(mirror, k)
            send_front_at(k)
            send_near_at(k)

    @pl.when(outer)
    def _():
        filter_quarter(across)
        send_quarter(across)

    total = length * rows
    target_at = lax.broadcasted_iota(jnp.int32, (total, length), 0) // rows
    lane = lax.broadcasted_iota(jnp.int32, (total, length), 1)
    spread = jnp.sum(
        jnp.where(target_at == lane, widths_ref[...], 0.0), axis=1, keepdims=True
    )
    row_at = lax.broadcasted_iota(jnp.int32, (total, total), 0)
    col_at = lax.broadcasted_iota(jnp.int32, (total, total), 1)
    apart = row_at // rows - col_at // rows
    inside = (jnp.abs(apart) <= BAND) & (row_at % rows == col_at % rows)
    offset = apart.astype(jnp.float32)
    weights = jnp.where(
        inside, jnp.exp(-offset * offset / (2.0 * spread * spread)), 0.0
    )
    weights = weights / jnp.sum(weights, axis=1, keepdims=True)
    depth = total // LAYERS
    high = weights.astype(jnp.bfloat16)
    low = (weights - high.astype(jnp.float32)).astype(jnp.bfloat16)
    for layer in range(LAYERS):
        at = slice(layer * depth, (layer + 1) * depth)
        mixing[layer, :, 0:depth] = high[:, at]
        mixing[layer, :, depth : 2 * depth] = high[:, at]
        mixing[layer, :, 2 * depth : 3 * depth] = low[:, at]

    last_ref[...] = mixing[mirror]

    def arrive(k, layer):
        block = incoming.at[k, pl.ds(layer * quarter, quarter)]
        pltpu.make_async_copy(block, block, recv_sem.at[k, layer]).wait()
        return block

    def share(k, layer):
        block = arrive(k, layer)
        if rows_block % 8 == 0:
            value = block[...].reshape(depth, chunk)
        else:
            value = jnp.concatenate([block[s] for s in range(quarter)], axis=0)
        return product(mixing[layer], value)

    def put(k, value):
        out_ref[:, :, pl.ds(pl.multiple_of(k * chunk, 128), chunk)] = value.reshape(
            length, rows, chunk
        )

    @pl.loop(0, chunks)
    def _(k):
        partial[...] = share(k, mine)
        partial[...] += share(k, beside)

        @pl.when(k < chunks - 1)
        def _():
            partial[...] += share(k, across)
            put(k, partial[...] + share(k, mirror))

        @pl.when(k == chunks - 1)
        def _():
            put(k, partial[...] + share(k, across))

    block = arrive(chunks - 1, mirror)
    if rows_block % 8 == 0:
        value = block[...].reshape(depth, chunk)
    else:
        value = jnp.concatenate([block[s] for s in range(quarter)], axis=0)
    rest_ref[...] = value

    @pl.loop(0, chunks)
    def _(k):
        sent = outgoing.at[k, pl.ds(0, n - 1)]
        pltpu.make_async_copy(sent, sent, send_sem.at[k]).wait()


def product(weights, value):
    high = value.astype(jnp.bfloat16)
    low = (value - high.astype(jnp.float32)).astype(jnp.bfloat16)
    return jnp.dot(
        weights,
        jnp.concatenate([high, low, high], axis=0),
        preferred_element_type=jnp.float32,
    )


def write_kernel(mixed_ref, last_ref, rest_ref, out_ref, end, sem):
    length, rows, columns = mixed_ref.shape
    chunk = rest_ref.shape[1]
    begin = columns - chunk
    ready = pltpu.make_async_copy(
        mixed_ref.at[:, :, pl.ds(0, begin)],
        out_ref.at[:, :, pl.ds(0, begin)],
        sem.at[0],
    )
    ready.start()
    end[...] = mixed_ref[:, :, begin:] + product(
        last_ref[...], rest_ref[...]
    ).reshape(length, rows, chunk)
    final = pltpu.make_async_copy(end, out_ref.at[:, :, pl.ds(begin, chunk)], sem.at[1])
    final.start()
    ready.wait()
    final.wait()


def in_hbm(array):
    return pltpu.with_memory_space_constraint(array, pltpu.HBM)


def local(n, frames, widths, kernel):
    per_device, height, columns = frames.shape
    length = widths.shape[0]
    rows = height // n
    chunk = 256 if columns % 256 == 0 else 128
    chunks = columns // chunk
    total = length * rows
    depth = total // LAYERS
    hbm = pl.BlockSpec(memory_space=pltpu.HBM)
    vmem = pl.BlockSpec(memory_space=pltpu.VMEM)
    shape = (length, rows, columns)
    rounds = 2 * (n // LAYERS).bit_length() + 1
    mixed = pl.pallas_call(
        functools.partial(exchange_kernel, n),
        out_shape=(
            pltpu.VMEM(shape, jnp.float32),
            pltpu.VMEM((total, 3 * depth), jnp.bfloat16),
            pltpu.VMEM((depth, chunk), jnp.float32),
        ),
        in_specs=[hbm] * 3,
        out_specs=(vmem, vmem, vmem),
        scratch_shapes=[
            pltpu.VMEM((per_device, height + 16, columns), jnp.float32),
            pltpu.VMEM((per_device, height // LAYERS + 16, columns), jnp.float32),
            pltpu.VMEM((per_device, 24, columns), jnp.float32),
            pltpu.VMEM((chunks, n, per_device * rows, chunk), jnp.float32),
            pltpu.VMEM((chunks, n, per_device * rows, chunk), jnp.float32),
            pltpu.VMEM((LAYERS, total, 3 * total // LAYERS), jnp.bfloat16),
            pltpu.VMEM((total, chunk), jnp.float32),
            pltpu.VMEM((1, length), jnp.float32),
            pltpu.SMEM((3, 3), jnp.float32),
            pltpu.SemaphoreType.DMA((6,)),
            pltpu.SemaphoreType.DMA((chunks,)),
            pltpu.SemaphoreType.DMA((chunks, LAYERS)),
            pltpu.SemaphoreType.REGULAR((rounds,)),
        ],
        compiler_params=pltpu.CompilerParams(
            collective_id=0,
            has_side_effects=True,
            vmem_limit_bytes=50 * 1024 * 1024,
        ),
    )(in_hbm(frames), in_hbm(widths.reshape(1, length)), in_hbm(kernel))
    return pl.pallas_call(
        write_kernel,
        out_shape=pltpu.HBM(shape, jnp.float32),
        in_specs=[vmem] * 3,
        out_specs=hbm,
        scratch_shapes=[
            pltpu.VMEM((length, rows, chunk), jnp.float32),
            pltpu.SemaphoreType.DMA((2,)),
        ],
        compiler_params=pltpu.CompilerParams(vmem_limit_bytes=4 * 1024 * 1024),
    )(*mixed)


def solution(mesh):
    return jax.shard_map(
        functools.partial(local, mesh.shape["blk"]),
        mesh=mesh,
        in_specs=(P("blk", None, None), P(), P()),
        out_specs=P(None, "blk", None),
        check_vma=False,
    )
```

```python
import functools

import jax
import jax.numpy as jnp
from jax import lax
from jax.experimental import pallas as pl
from jax.experimental.pallas import tpu as pltpu
from jax.sharding import PartitionSpec as P

BAND = 24
LAYERS = 4
MESH = pl.DeviceIdType.MESH


def exchange_kernel(
    n,
    frames_ref,
    widths_hbm,
    kernel_hbm,
    out_ref,
    last_ref,
    rest_ref,
    held,
    window,
    opening,
    outgoing,
    incoming,
    mixing,
    partial,
    widths_ref,
    kernel_ref,
    in_sem,
    send_sem,
    recv_sem,
    round_sem,
):
    per_device, height, columns = frames_ref.shape
    chunks, _, rows_block, chunk = outgoing.shape
    rows = rows_block // per_device
    group = 8 // rows
    held_back = max(chunks - 1, 1)
    length = widths_ref.shape[1]
    me = lax.axis_index("blk")
    quarter = n // LAYERS
    mine = me // quarter
    place = me - mine * quarter
    mirror = 3 - mine
    beside = mine + 1 - 2 * lax.rem(mine, 2)
    across = mirror + 1 - 2 * lax.rem(mirror, 2)
    inner = (mine == 1) | (mine == 2)
    outer = jnp.logical_not(inner)
    front = jnp.where(inner, mirror, beside)
    opposite = mirror * quarter + place
    partner = beside * quarter + place
    part = quarter // group
    seat = place // group
    member_of = place - seat * group
    bits = part.bit_length() - 1
    core_bits = group.bit_length() - 1
    steps = core_bits + bits
    arrived = round_sem.at[2 * steps]
    meet = round_sem.at[2 * steps + 1]
    relay = round_sem.at[2 * steps + 2]

    def flip(value, step):
        return value + step - 2 * step * lax.rem(value // step, 2)

    def mixed_seat(step):
        return lax.rem(seat + step, part)

    def crossed_seat(step):
        total = 0
        for bit in range(bits):
            width = 1 << bit
            total = total + width * lax.rem(seat // width + step // width, 2)
        return total

    own = front * part + seat
    strip = height // LAYERS
    first = front * strip

    def load(source, rows_in, target, at, semaphore):
        return pltpu.make_async_copy(
            frames_ref.at[:, pl.ds(pl.multiple_of(source, 8), rows_in), :],
            target.at[:, pl.ds(at, rows_in), :],
            semaphore,
        )

    taps_load = pltpu.make_async_copy(kernel_hbm, kernel_ref, in_sem.at[0])
    top = pl.multiple_of(first + seat * 8 - 8, 8)
    margin = min(chunk + 128, columns)
    edges = [(0, margin)] + ([(margin, columns)] if margin < columns else [])
    early = [
        pltpu.make_async_copy(
            frames_ref.at[:, pl.ds(top, 24), pl.ds(begin, end - begin)],
            opening.at[:, :, pl.ds(begin, end - begin)],
            in_sem.at[4 + at],
        )
        for at, (begin, end) in enumerate(edges)
    ]
    front_load = load(first - 8, strip + 16, window, 0, in_sem.at[1])
    late = [
        load(0, height, held, 8, in_sem.at[2]),
        pltpu.make_async_copy(widths_hbm, widths_ref, in_sem.at[3]),
    ]
    taps_load.start()
    for copy in early:
        copy.start()
    front_load.start()

    def signal(semaphore, target):
        pl.semaphore_signal(
            semaphore, inc=1, device_id=(target,), device_id_type=MESH
        )

    barrier = pltpu.get_barrier_semaphore()
    neighbours = [flip(place, 1 << bit) for bit in range(core_bits + bits)]
    for place_at in neighbours:
        signal(barrier, mine * quarter + place_at)

    @pl.when(inner)
    def _():
        for layer in (mirror, beside):
            for member in range(group):
                signal(barrier, layer * quarter + seat * group + member)

    edge = jnp.zeros((per_device, 8, columns), jnp.float32)
    held[:, pl.ds(0, 8), :] = edge
    held[:, pl.ds(height + 8, 8), :] = edge

    def filter_frame(at, source, frame, start, begin=0, end=None):
        end = columns if end is None else end
        low, high = max(begin - 128, 0), min(end + 128, columns)
        wide = high - low
        tall = source[frame, pl.ds(start, 24), low:high]
        taps = [tall[7:15], tall[8:16], tall[9:17]]
        mixed = [
            kernel_ref[0, col] * taps[0]
            + kernel_ref[1, col] * taps[1]
            + kernel_ref[2, col] * taps[2]
            for col in range(3)
        ]
        left = pltpu.roll(mixed[0], 1, 1)
        right = pltpu.roll(mixed[2], wide - 1, 1)
        lane = lax.broadcasted_iota(jnp.int32, (8, wide), 1) + low
        if low == 0:
            left = jnp.where(lane == 0, 0.0, left)
        if high == columns:
            right = jnp.where(lane == columns - 1, 0.0, right)
        value = left + mixed[1] + right
        for member in range(group):
            for k in range(begin // chunk, end // chunk):
                outgoing[
                    k, at * group + member, pl.ds(frame * rows, rows), :
                ] = value[
                    member * rows : (member + 1) * rows,
                    k * chunk - low : (k + 1) * chunk - low,
                ]

    def filter_group(at, source, base):
        start = pl.multiple_of((at - base) * 8, 8)
        for frame in range(per_device):
            filter_frame(at, source, frame, start)

    def send(k, target):
        pltpu.make_async_remote_copy(
            src_ref=outgoing.at[k, target],
            dst_ref=incoming.at[k, me],
            send_sem=send_sem.at[k],
            recv_sem=recv_sem.at[k, mine],
            device_id=(target,),
            device_id_type=MESH,
        ).start()

    def send_group(at):
        @pl.loop(1, held_back)
        def _(k):
            for member in range(group):
                send(k, at * group + member)

    def send_quarter_at(which, k):
        @pl.loop(0, part)
        def _(step):
            at = which * part + lax.rem(seat + part + step * (1 - 2 * lax.rem(me, 2)), part)
            for member in range(group):
                send(k, at * group + member)

    def send_quarter(which):
        @pl.loop(0, chunks)
        def _(k):
            send_quarter_at(which, k)

    def send_front_at(k):
        @pl.loop(1, part)
        def _(step):
            seat_at = jnp.where(
                k >= held_back, crossed_seat(part - step), mixed_seat(step)
            )
            at = front * part + seat_at
            for member in range(group):
                send(k, at * group + member)

        @pl.when(outer | (k >= held_back))
        def _():
            for member in reversed(range(group)):
                send(k, own * group + member)

    def send_front(begin, end):
        @pl.loop(begin, end)
        def _(k):
            send_front_at(k)

    def send_near_at(k):
        @pl.loop(1, part)
        def _(step):
            at = mine * part + mixed_seat(step)
            for member in range(group):
                send(k, at * group + member)

        for other in range(1, group):
            send(
                k,
                mine * quarter
                + seat * group
                + lax.rem(member_of + other, group),
            )
        pltpu.make_async_copy(
            outgoing.at[k, me], incoming.at[k, me], recv_sem.at[k, mine]
        ).start()

    def filter_quarter(which):
        @pl.loop(0, part)
        def _(step):
            filter_group(which * part + mixed_seat(step), held, 0)

    taps_load.wait()
    early[0].wait()
    for frame in range(per_device):
        filter_frame(own, opening, frame, 0, 0, chunk)
    pl.semaphore_wait(barrier, group + steps)

    @pl.when(inner)
    def _():
        for member in range(group):
            send(0, own * group + member)

    if chunks > 1:
        early[-1].wait()
        for frame in range(per_device):
            filter_frame(own, opening, frame, 0, chunk, columns)
        pl.when(inner)(lambda: send_group(own))
    for copy in late:
        copy.start()

    @pl.when(outer)
    def _():
        signal(arrived, partner)

    def pass_on(bit, at):
        signal(at, mine * quarter + neighbours[bit])

    for bit in range(core_bits):
        pass_on(bit, round_sem.at[bit])
        pl.semaphore_wait(round_sem.at[bit], 1)
    for bit in range(bits):
        at = round_sem.at[core_bits + bit]
        pass_on(core_bits + bit, at)
        if bit == 0:
            front_load.wait()

        @pl.loop(1 << bit, 2 << bit)
        def _(step):
            filter_group(front * part + crossed_seat(step), window, front * part)

        pl.semaphore_wait(at, 1)

        @pl.when(inner)
        def _():
            @pl.loop(1 << bit, 2 << bit)
            def _(step):
                for member in range(group):
                    send(0, (front * part + crossed_seat(step)) * group + member)

    split = jnp.where(inner, min(2, chunks), 0)
    send_front(1, split)
    for copy in late:
        copy.wait()

    @pl.when(inner)
    def _():
        pl.semaphore_wait(arrived, 1)
        for bit in range(steps):
            at = round_sem.at[steps + bit]
            pass_on(bit, at)
            if bit < part:
                filter_group(across * part + mixed_seat(bit), held, 0)
            pl.semaphore_wait(at, 1)
        signal(meet, opposite)

        @pl.loop(min(steps, part), part)
        def _(step):
            filter_group(across * part + mixed_seat(step), held, 0)

        pl.semaphore_wait(meet, 1)
        signal(relay, partner)
        filter_quarter(mine)
        send_quarter(across)

    pl.when(outer)(lambda: filter_quarter(mine))

    @pl.when(inner)
    def _():
        filter_quarter(beside)

        @pl.loop(0, chunks)
        def _(k):
            send_quarter_at(beside, k)
            send_near_at(k)

        send_front(split, chunks)

    @pl.when(outer)
    def _():
        filter_quarter(mirror)
        pl.semaphore_wait(relay, 1)

        @pl.loop(0, chunks)
        def _(k):
            send_quarter_at(mirror, k)
            send_front_at(k)
            send_near_at(k)

    @pl.when(outer)
    def _():
        filter_quarter(across)
        send_quarter(across)

    total = length * rows
    target_at = lax.broadcasted_iota(jnp.int32, (total, length), 0) // rows
    lane = lax.broadcasted_iota(jnp.int32, (total, length), 1)
    spread = jnp.sum(
        jnp.where(target_at == lane, widths_ref[...], 0.0), axis=1, keepdims=True
    )
    row_at = lax.broadcasted_iota(jnp.int32, (total, total), 0)
    col_at = lax.broadcasted_iota(jnp.int32, (total, total), 1)
    apart = row_at // rows - col_at // rows
    inside = (jnp.abs(apart) <= BAND) & (row_at % rows == col_at % rows)
    offset = apart.astype(jnp.float32)
    weights = jnp.where(
        inside, jnp.exp(-offset * offset / (2.0 * spread * spread)), 0.0
    )
    weights = weights / jnp.sum(weights, axis=1, keepdims=True)
    depth = total // LAYERS
    high = weights.astype(jnp.bfloat16)
    low = (weights - high.astype(jnp.float32)).astype(jnp.bfloat16)
    for layer in range(LAYERS):
        at = slice(layer * depth, (layer + 1) * depth)
        mixing[layer, :, 0:depth] = high[:, at]
        mixing[layer, :, depth : 2 * depth] = high[:, at]
        mixing[layer, :, 2 * depth : 3 * depth] = low[:, at]

    last_ref[...] = mixing[mirror]

    def arrive(k, layer):
        block = incoming.at[k, pl.ds(layer * quarter, quarter)]
        pltpu.make_async_copy(block, block, recv_sem.at[k, layer]).wait()
        return block

    def share(k, layer):
        block = arrive(k, layer)
        if rows_block % 8 == 0:
            value = block[...].reshape(depth, chunk)
        else:
            value = jnp.concatenate([block[s] for s in range(quarter)], axis=0)
        return product(mixing[layer], value)

    def put(k, value):
        out_ref[:, :, pl.ds(pl.multiple_of(k * chunk, 128), chunk)] = value.reshape(
            length, rows, chunk
        )

    @pl.loop(0, chunks)
    def _(k):
        partial[...] = share(k, mine)
        partial[...] += share(k, beside)

        @pl.when(k < chunks - 1)
        def _():
            partial[...] += share(k, across)
            put(k, partial[...] + share(k, mirror))

        @pl.when(k == chunks - 1)
        def _():
            put(k, partial[...] + share(k, across))

    @pl.loop(0, chunks)
    def _(k):
        sent = outgoing.at[k, pl.ds(0, n - 1)]
        pltpu.make_async_copy(sent, sent, send_sem.at[k]).wait()

    block = arrive(chunks - 1, mirror)
    if rows_block % 8 == 0:
        value = block[...].reshape(depth, chunk)
    else:
        value = jnp.concatenate([block[s] for s in range(quarter)], axis=0)
    rest_ref[...] = value


def product(weights, value):
    high = value.astype(jnp.bfloat16)
    low = (value - high.astype(jnp.float32)).astype(jnp.bfloat16)
    return jnp.dot(
        weights,
        jnp.concatenate([high, low, high], axis=0),
        preferred_element_type=jnp.float32,
    )


def write_kernel(mixed_ref, last_ref, rest_ref, out_ref, end, sem):
    length, rows, columns = mixed_ref.shape
    chunk = rest_ref.shape[1]
    begin = columns - chunk
    ready = pltpu.make_async_copy(
        mixed_ref.at[:, :, pl.ds(0, begin)],
        out_ref.at[:, :, pl.ds(0, begin)],
        sem.at[0],
    )
    ready.start()
    end[...] = mixed_ref[:, :, begin:] + product(
        last_ref[...], rest_ref[...]
    ).reshape(length, rows, chunk)
    final = pltpu.make_async_copy(end, out_ref.at[:, :, pl.ds(begin, chunk)], sem.at[1])
    final.start()
    ready.wait()
    final.wait()


def in_hbm(array):
    return pltpu.with_memory_space_constraint(array, pltpu.HBM)


def local(n, frames, widths, kernel):
    per_device, height, columns = frames.shape
    length = widths.shape[0]
    rows = height // n
    chunk = 256 if columns % 256 == 0 else 128
    chunks = columns // chunk
    total = length * rows
    depth = total // LAYERS
    hbm = pl.BlockSpec(memory_space=pltpu.HBM)
    vmem = pl.BlockSpec(memory_space=pltpu.VMEM)
    shape = (length, rows, columns)
    rounds = 2 * (n // LAYERS).bit_length() + 1
    mixed = pl.pallas_call(
        functools.partial(exchange_kernel, n),
        out_shape=(
            pltpu.VMEM(shape, jnp.float32),
            pltpu.VMEM((total, 3 * depth), jnp.bfloat16),
            pltpu.VMEM((depth, chunk), jnp.float32),
        ),
        in_specs=[hbm] * 3,
        out_specs=(vmem, vmem, vmem),
        scratch_shapes=[
            pltpu.VMEM((per_device, height + 16, columns), jnp.float32),
            pltpu.VMEM((per_device, height // LAYERS + 16, columns), jnp.float32),
            pltpu.VMEM((per_device, 24, columns), jnp.float32),
            pltpu.VMEM((chunks, n, per_device * rows, chunk), jnp.float32),
            pltpu.VMEM((chunks, n, per_device * rows, chunk), jnp.float32),
            pltpu.VMEM((LAYERS, total, 3 * total // LAYERS), jnp.bfloat16),
            pltpu.VMEM((total, chunk), jnp.float32),
            pltpu.VMEM((1, length), jnp.float32),
            pltpu.SMEM((3, 3), jnp.float32),
            pltpu.SemaphoreType.DMA((6,)),
            pltpu.SemaphoreType.DMA((chunks,)),
            pltpu.SemaphoreType.DMA((chunks, LAYERS)),
            pltpu.SemaphoreType.REGULAR((rounds,)),
        ],
        compiler_params=pltpu.CompilerParams(
            collective_id=0,
            has_side_effects=True,
            vmem_limit_bytes=50 * 1024 * 1024,
        ),
    )(in_hbm(frames), in_hbm(widths.reshape(1, length)), in_hbm(kernel))
    return pl.pallas_call(
        write_kernel,
        out_shape=pltpu.HBM(shape, jnp.float32),
        in_specs=[vmem] * 3,
        out_specs=hbm,
        scratch_shapes=[
            pltpu.VMEM((length, rows, chunk), jnp.float32),
            pltpu.SemaphoreType.DMA((2,)),
        ],
        compiler_params=pltpu.CompilerParams(vmem_limit_bytes=4 * 1024 * 1024),
    )(*mixed)


def solution(mesh):
    return jax.shard_map(
        functools.partial(local, mesh.shape["blk"]),
        mesh=mesh,
        in_specs=(P("blk", None, None), P(), P()),
        out_specs=P(None, "blk", None),
        check_vma=False,
    )
```
